32 devices in a mesh: expert: 4 (over y, core), shard: 8 (over z, x).
Axes of the slice: x: 2, y: 2, z: 4, core: 2. Of those that a mesh axis runs over, the one named last changes fastest.
Arguments:
- master_gate: float32 [128, 2048, 768], P('expert', 'shard'), may hold values from -0.125 to 0.125
- second_gate: bfloat16 [128, 2048, 768], P('expert', 'shard'), may hold values from -0.0625 to 0.0625
- master_up: float32 [128, 2048, 768], P('expert', 'shard'), may hold values from -0.125 to 0.125
- second_up: bfloat16 [128, 2048, 768], P('expert', 'shard'), may hold values from -0.0625 to 0.0625
- router_weight: float32 [2048, 128], P('shard', 'expert'), may hold values from -0.125 to 0.125
- router_gain: float32 [2048], P('shard'), may hold values from 0.25 to 1.75
Outputs:
- final_gate: bfloat16 [128, 768, 2048], P('expert', 'shard')
- final_up: bfloat16 [128, 768, 2048], P('expert', 'shard')
- serve_router: bfloat16 [2048, 128], replicated
The draws below stay inside these ranges and needn't reach their ends.
All inputs are finite; a program needn't handle non-finite values.
Results may differ from the reference program's by a relative error of at most 0.001.
Values may be sent and summed in bfloat16 or wider, within the bound.
A program may use at most 192 MiB of HBM per device.

```python
import jax
import jax.numpy as jnp

EXPERTS = 128
D_MODEL = 2048
D_EXPERT = 768


def levels(rng, dims, split, low, high):
    def one(position, shards_of):
        draws = jax.random.uniform(jax.random.fold_in(jax.random.fold_in(rng, 6), position), (shards_of,), jnp.float32, low / len(split), high / len(split))
        return jnp.repeat(jnp.exp(draws), dims[position] // shards_of).reshape((-1,) + (1,) * (len(dims) - position - 1))

    gain = one(*split[0])
    for cut in split[1:]:
        gain = gain * one(*cut)
    return gain


def scatter_about(stream_key, shape, spread, most, cuts=(), held_as=jnp.bfloat16):
    array = jax.random.normal(stream_key, shape, jnp.float32) * spread
    if len(cuts) > 0:
        array = levels(stream_key, shape, cuts, -0.22, 0.18) * array
    return jnp.clip(array, min=-most, max=most).astype(held_as)


def setup_inputs(seed: int = 0) -> dict:
    arg_keys = jax.random.split(jax.random.key(seed), 7)
    master_gate = scatter_about(arg_keys[0], (EXPERTS, D_MODEL, D_EXPERT), D_MODEL ** -0.5, 0.125, ((0, 4), (1, 8)), jnp.float32)
    second_gate = scatter_about(arg_keys[1], (EXPERTS, D_MODEL, D_EXPERT), (D_MODEL * 4) ** -0.5, 0.0625, ((0, 4), (1, 8)))
    master_up = scatter_about(arg_keys[2], (EXPERTS, D_MODEL, D_EXPERT), D_MODEL ** -0.5, 0.125, ((0, 4), (1, 8)), jnp.float32)
    second_up = scatter_about(arg_keys[3], (EXPERTS, D_MODEL, D_EXPERT), (D_MODEL * 4) ** -0.5, 0.0625, ((0, 4), (1, 8)))
    router_weight = scatter_about(arg_keys[4], (D_MODEL, EXPERTS), D_MODEL ** -0.5, 0.125, ((0, 8), (1, 4)), jnp.float32)
    router_gain = jnp.clip(1.0 + 0.15 * jax.random.normal(arg_keys[5], (D_MODEL,), jnp.float32), 0.25, 1.75)
    return dict(master_gate=master_gate, second_gate=second_gate, master_up=master_up, second_up=second_up, router_weight=router_weight, router_gain=router_gain)


def reference(master_gate, second_gate, master_up, second_up, router_weight, router_gain):
    merged_gate = master_gate + second_gate.astype(jnp.float32)
    merged_up = master_up + second_up.astype(jnp.float32)
    final_gate = merged_gate.astype(jnp.bfloat16)
    final_gate = jnp.transpose(final_gate, (0, 2, 1))
    final_up = merged_up.astype(jnp.bfloat16)
    final_up = jnp.transpose(final_up, (0, 2, 1))
    serve_router = (router_weight * router_gain[:, None]).astype(jnp.bfloat16)
    return final_gate, final_up, serve_router
```

```python
import functools

import jax
import jax.numpy as jnp
from jax import lax
from jax.experimental import pallas as pl
from jax.experimental.pallas import tpu as pltpu
from jax.sharding import PartitionSpec as P

SLOTS = 12
LOADS = 2
MESH_IDS = pl.DeviceIdType.MESH


def plain(master_gate, second_gate, master_up, second_up, router_weight, router_gain):
    merged_gate = master_gate + second_gate.astype(jnp.float32)
    merged_up = master_up + second_up.astype(jnp.float32)
    narrow_gate, narrow_up = (merged_gate.astype(jnp.bfloat16), merged_up.astype(jnp.bfloat16))
    final_gate, final_up = (
        lax.all_to_all(narrow_gate, "shard", split_axis=2, concat_axis=1, tiled=True),
        lax.all_to_all(narrow_up, "shard", split_axis=2, concat_axis=1, tiled=True),
    )
    final_gate = jnp.transpose(final_gate, (0, 2, 1))
    final_up = jnp.transpose(final_up, (0, 2, 1))
    part_router = (router_weight * router_gain[:, None]).astype(jnp.bfloat16)
    row_router = lax.all_gather(part_router, "shard", axis=0, tiled=True)
    serve_router = lax.all_gather(row_router, "expert", axis=1, tiled=True)
    return (final_gate, final_up, serve_router)


def peers(me, n):
    half = n // 2
    mine, place = me // half, me % half
    far = [(1 - mine) * half + (place + i) % half for i in range(half)]
    near = [mine * half + (place + i) % half for i in range(1, half)]
    return far + near


def regroup_kernel(n, groups, mg, sg, mu, su, rw, gain, og, ou, orr,
                   in_m, in_s, stage, rw_v, gain_v, r_part, r_all,
                   load_m, load_s, load_r, send, own, recv, r_send, r_recv, f_send, f_recv):
    experts, rows, inner = mg.shape
    part = inner // n
    r_cols = rw.shape[0]
    group, me = lax.axis_index("expert"), lax.axis_index("shard")
    to = peers(me, n)
    other = [(group + i) % groups for i in range(1, groups)]
    masters, seconds, outs = (mg, mu), (sg, su), (og, ou)
    home = pl.ds(pl.multiple_of(me * rows, rows), rows)

    def loads(a, e):
        slot = e % LOADS
        return (
            pltpu.make_async_copy(masters[a].at[e], in_m.at[a, slot], load_m.at[a, slot]),
            pltpu.make_async_copy(seconds[a].at[e], in_s.at[a, slot], load_s.at[a, slot]),
        )

    def start_loads(a, e):
        for copy in loads(a, e):
            copy.start()

    def router_loads():
        return (
            pltpu.make_async_copy(rw, rw_v, load_r.at[0]),
            pltpu.make_async_copy(gain, gain_v, load_r.at[1]),
        )

    def block(a, e, device):
        src = pl.ds(pl.multiple_of(device * part, part), part)
        return stage.at[a, e % SLOTS, src, :], outs[a].at[e, :, home]

    def start_sends(a, e):
        for device in to:
            src, dst = block(a, e, device)
            pltpu.make_async_remote_copy(
                src_ref=src, dst_ref=dst, send_sem=send.at[a, e % SLOTS], recv_sem=recv.at[a, e],
                device_id=(group, device), device_id_type=MESH_IDS,
            ).start()
        src, dst = block(a, e, me)
        pltpu.make_async_copy(src, dst, own.at[a, e % SLOTS]).start()

    def wait_sends(a, e):
        many = stage.at[a, e % SLOTS, pl.ds(0, (n - 1) * part), :]
        pltpu.make_async_copy(many, many, send.at[a, e % SLOTS]).wait()
        src, dst = block(a, e, me)
        pltpu.make_async_copy(src, dst, own.at[a, e % SLOTS]).wait()

    def merge(a, e):
        for copy in loads(a, e):
            copy.wait()

        @pl.when(e >= SLOTS)
        def _():
            wait_sends(a, e - SLOTS)

        slot, into = e % LOADS, e % SLOTS
        for c in range(inner // 128):
            cols = slice(c * 128, (c + 1) * 128)
            merged = in_m[a, slot, :, cols] + in_s[a, slot, :, cols].astype(jnp.float32)
            stage[a, into, cols, :] = merged.T.astype(jnp.bfloat16)

        @pl.when(e + LOADS < experts)
        def _():
            start_loads(a, e + LOADS)

    for a in range(2):
        start_loads(a, 0)
    for copy in router_loads():
        copy.start()
    for e in range(1, LOADS):
        for a in range(2):
            start_loads(a, e)

    barrier = pltpu.get_barrier_semaphore()
    for device in to:
        pl.semaphore_signal(barrier, inc=1, device_id=(group, device), device_id_type=MESH_IDS)
    for g in other:
        pl.semaphore_signal(barrier, inc=1, device_id=(g, me), device_id_type=MESH_IDS)

    merge(0, 0)
    for copy in router_loads():
        copy.wait()
    mine = (rw_v[...] * gain_v[...]).astype(jnp.bfloat16)
    r_rows = pl.ds(pl.multiple_of(group * r_cols, r_cols), r_cols)
    r_part[...] = mine
    r_all[r_rows, home] = mine
    pl.semaphore_wait(barrier, len(to) + len(other))

    def after_first(e):
        merge(1, e)
        start_sends(0, e)

    after_first(0)
    for device in to:
        pltpu.make_async_remote_copy(
            src_ref=r_part, dst_ref=r_all.at[r_rows, home], send_sem=r_send, recv_sem=r_recv,
            device_id=(group, device), device_id_type=MESH_IDS,
        ).start()

    def step(e, carry):
        merge(0, e)
        start_sends(1, e - 1)
        after_first(e)
        return carry

    lax.fori_loop(1, experts, step, 0)

    many = r_all.at[pl.ds(0, r_cols), pl.ds(0, (n - 1) * rows)]
    pltpu.make_async_copy(many, many, r_recv).wait()
    pltpu.make_async_copy(many, many, r_send).wait()
    start_sends(1, experts - 1)
    for g in other:
        pltpu.make_async_remote_copy(
            src_ref=r_all.at[r_rows, :], dst_ref=r_all.at[r_rows, :], send_sem=f_send, recv_sem=f_recv,
            device_id=(g, me), device_id_type=MESH_IDS,
        ).start()
    many = r_all.at[pl.ds(0, (groups - 1) * r_cols), :]
    pltpu.make_async_copy(many, many, f_recv).wait()
    pltpu.make_async_copy(many, many, f_send).wait()
    for c in range(orr.shape[0] // 128):
        span = slice(c * 128, (c + 1) * 128)
        orr[span, :] = r_all[:, span].astype(jnp.float32).T.astype(jnp.bfloat16)

    def drain(e, carry):
        for a in range(2):
            wait_sends(a, e)
        return carry

    lax.fori_loop(max(experts - SLOTS, 0), experts, drain, 0)

    def arrive(e, carry):
        for a in range(2):
            many = outs[a].at[e, :, pl.ds(0, (n - 1) * rows)]
            pltpu.make_async_copy(many, many, recv.at[a, e]).wait()
        return carry

    lax.fori_loop(0, experts, arrive, 0)


def put_kernel(gate, up, router, og, ou, orr, done):
    copies = [
        pltpu.make_async_copy(src, dst, done.at[i])
        for i, (src, dst) in enumerate(((gate, og), (up, ou), (router, orr)))
    ]
    for copy in copies:
        copy.start()
    for copy in copies:
        copy.wait()


def put(*held):
    anywhere = pl.BlockSpec(memory_space=pl.ANY)
    return pl.pallas_call(
        put_kernel,
        out_shape=tuple(pltpu.HBM(x.shape, x.dtype) for x in held),
        in_specs=[anywhere] * len(held),
        out_specs=(anywhere,) * len(held),
        scratch_shapes=[pltpu.SemaphoreType.DMA((len(held),))],
        compiler_params=pltpu.CompilerParams(vmem_limit_bytes=1024 * 1024),
        name="put",
    )(*held)


def fused(n, groups, master_gate, second_gate, master_up, second_up, router_weight, router_gain):
    experts, rows, inner = master_gate.shape
    r_cols = router_weight.shape[1]
    final = (experts, inner // n, rows * n)
    anywhere = pl.BlockSpec(memory_space=pl.ANY)
    dma = pltpu.SemaphoreType.DMA
    return put(*pl.pallas_call(
        functools.partial(regroup_kernel, n, groups),
        out_shape=(
            pltpu.VMEM(final, jnp.bfloat16),
            pltpu.VMEM(final, jnp.bfloat16),
            jax.ShapeDtypeStruct((rows * n, r_cols * groups), jnp.bfloat16),
        ),
        in_specs=[anywhere] * 6,
        out_specs=(anywhere, anywhere, pl.BlockSpec(memory_space=pltpu.VMEM)),
        scratch_shapes=[
            pltpu.VMEM((2, LOADS, rows, inner), jnp.float32),
            pltpu.VMEM((2, LOADS, rows, inner), jnp.bfloat16),
            pltpu.VMEM((2, SLOTS, inner, rows), jnp.bfloat16),
            pltpu.VMEM((r_cols, rows), jnp.float32),
            pltpu.VMEM((1, rows), jnp.float32),
            pltpu.VMEM((r_cols, rows), jnp.bfloat16),
            pltpu.VMEM((r_cols * groups, rows * n), jnp.bfloat16),
            dma((2, LOADS)), dma((2, LOADS)), dma((2,)),
            dma((2, SLOTS)), dma((2, SLOTS)), dma((2, experts)),
            dma, dma, dma, dma,
        ],
        compiler_params=pltpu.CompilerParams(
            collective_id=0, has_side_effects=True, vmem_limit_bytes=24 * 1024 * 1024,
        ),
        name="regroup",
    )(master_gate, second_gate, master_up, second_up, router_weight.T, router_gain[None, :]))


def solution(mesh):
    n, groups = mesh.shape["shard"], mesh.shape["expert"]

    def shards(*args):
        experts, rows, inner = args[0].shape
        r_cols = args[4].shape[1]
        fits = (
            n % 2 == 0 and groups > 1 and rows % 128 == 0 and inner % 128 == 0
            and (inner // n) % 16 == 0 and r_cols % 16 == 0 and experts >= max(SLOTS, LOADS)
        )
        return fused(n, groups, *args) if fits else plain(*args)

    in_specs = (
        P("expert", "shard", None),
        P("expert", "shard", None),
        P("expert", "shard", None),
        P("expert", "shard", None),
        P("shard", "expert"),
        P("shard"),
    )
    out_specs = (P("expert", "shard", None), P("expert", "shard", None), P())
    return jax.shard_map(shards, mesh=mesh, in_specs=in_specs, out_specs=out_specs, check_vma=False)
```

```python
import functools

import jax
import jax.numpy as jnp
from jax import lax
from jax.experimental import pallas as pl
from jax.experimental.pallas import tpu as pltpu
from jax.sharding import PartitionSpec as P

SLOTS = 12
LOADS = 2
MESH_IDS = pl.DeviceIdType.MESH


def plain(master_gate, second_gate, master_up, second_up, router_weight, router_gain):
    merged_gate = master_gate + second_gate.astype(jnp.float32)
    merged_up = master_up + second_up.astype(jnp.float32)
    narrow_gate, narrow_up = (merged_gate.astype(jnp.bfloat16), merged_up.astype(jnp.bfloat16))
    final_gate, final_up = (
        lax.all_to_all(narrow_gate, "shard", split_axis=2, concat_axis=1, tiled=True),
        lax.all_to_all(narrow_up, "shard", split_axis=2, concat_axis=1, tiled=True),
    )
    final_gate = jnp.transpose(final_gate, (0, 2, 1))
    final_up = jnp.transpose(final_up, (0, 2, 1))
    part_router = (router_weight * router_gain[:, None]).astype(jnp.bfloat16)
    row_router = lax.all_gather(part_router, "shard", axis=0, tiled=True)
    serve_router = lax.all_gather(row_router, "expert", axis=1, tiled=True)
    return (final_gate, final_up, serve_router)


def peers(me, n):
    half = n // 2
    mine, place = me // half, me % half
    far = [(1 - mine) * half + (place + i) % half for i in range(half)]
    near = [mine * half + (place + i) % half for i in range(1, half)]
    return far, near


def regroup_kernel(n, groups, mg, sg, mu, su, rw, gain, og, ou, orr,
                   in_m, in_s, stage, rw_v, gain_v, r_part, r_all,
                   load_m, load_s, load_r, send, own, recv, r_send, r_recv, f_send, f_recv):
    experts, rows, inner = mg.shape
    part = inner // n
    r_cols = rw.shape[0]
    group, me = lax.axis_index("expert"), lax.axis_index("shard")
    far, near = peers(me, n)
    to = far + near
    other = [(group + i) % groups for i in range(1, groups)]
    masters, seconds, outs = (mg, mu), (sg, su), (og, ou)
    home = pl.ds(pl.multiple_of(me * rows, rows), rows)

    def loads(a, e):
        slot = e % LOADS
        return (
            pltpu.make_async_copy(masters[a].at[e], in_m.at[a, slot], load_m.at[a, slot]),
            pltpu.make_async_copy(seconds[a].at[e], in_s.at[a, slot], load_s.at[a, slot]),
        )

    def start_loads(a, e):
        for copy in loads(a, e):
            copy.start()

    def router_loads():
        return (
            pltpu.make_async_copy(rw, rw_v, load_r.at[0]),
            pltpu.make_async_copy(gain, gain_v, load_r.at[1]),
        )

    def block(a, e, device):
        src = pl.ds(pl.multiple_of(device * part, part), part)
        return stage.at[a, e % SLOTS, src, :], outs[a].at[e, :, home]

    def start_sends(a, e):
        for device in to:
            src, dst = block(a, e, device)
            pltpu.make_async_remote_copy(
                src_ref=src, dst_ref=dst, send_sem=send.at[a, e % SLOTS], recv_sem=recv.at[a, e],
                device_id=(group, device), device_id_type=MESH_IDS,
            ).start()
        src, dst = block(a, e, me)
        pltpu.make_async_copy(src, dst, own.at[a, e % SLOTS]).start()

    def wait_sends(a, e):
        many = stage.at[a, e % SLOTS, pl.ds(0, (n - 1) * part), :]
        pltpu.make_async_copy(many, many, send.at[a, e % SLOTS]).wait()
        src, dst = block(a, e, me)
        pltpu.make_async_copy(src, dst, own.at[a, e % SLOTS]).wait()

    def merge(a, e):
        for copy in loads(a, e):
            copy.wait()

        @pl.when(e >= SLOTS)
        def _():
            wait_sends(a, e - SLOTS)

        slot, into = e % LOADS, e % SLOTS
        for c in range(inner // 128):
            cols = slice(c * 128, (c + 1) * 128)
            merged = in_m[a, slot, :, cols] + in_s[a, slot, :, cols].astype(jnp.float32)
            stage[a, into, cols, :] = merged.T.astype(jnp.bfloat16)

        @pl.when(e + LOADS < experts)
        def _():
            start_loads(a, e + LOADS)

    for a in range(2):
        start_loads(a, 0)
    for copy in router_loads():
        copy.start()
    for e in range(1, LOADS):
        for a in range(2):
            start_loads(a, e)

    barrier = pltpu.get_barrier_semaphore()
    for device in to:
        pl.semaphore_signal(barrier, inc=1, device_id=(group, device), device_id_type=MESH_IDS)
    for g in other:
        pl.semaphore_signal(barrier, inc=1, device_id=(g, me), device_id_type=MESH_IDS)

    merge(0, 0)
    for copy in router_loads():
        copy.wait()
    mine = (rw_v[...] * gain_v[...]).astype(jnp.bfloat16)
    r_rows = pl.ds(pl.multiple_of(group * r_cols, r_cols), r_cols)
    r_part[...] = mine
    r_all[r_rows, home] = mine
    pl.semaphore_wait(barrier, len(to) + len(other))
    start_sends(0, 0)
    merge(1, 0)

    def hand(src, dst, i, device):
        pltpu.make_async_remote_copy(
            src_ref=src, dst_ref=dst, send_sem=r_send.at[i], recv_sem=r_recv.at[i],
            device_id=(group, device), device_id_type=MESH_IDS,
        ).start()

    def wait_hands(sems, i, count):
        many = r_all.at[pl.ds(0, r_cols), pl.ds(0, count * rows)]
        pltpu.make_async_copy(many, many, sems.at[i]).wait()

    hand(r_part, r_all.at[r_rows, home], 0, far[0])
    for device in near:
        hand(r_part, r_all.at[r_rows, home], 1, device)

    def step(e, carry):
        merge(0, e)
        start_sends(1, e - 1)
        merge(1, e)
        start_sends(0, e)
        return carry

    lax.fori_loop(1, experts, step, 0)

    wait_hands(r_recv, 0, 1)
    mirror = r_all.at[r_rows, pl.ds(pl.multiple_of(far[0] * rows, rows), rows)]
    for device in near:
        hand(mirror, mirror, 2, device)
    start_sends(1, experts - 1)
    wait_hands(r_send, 0, 1)
    for i in (1, 2):
        wait_hands(r_recv, i, len(near))
        wait_hands(r_send, i, len(near))
    for g in other:
        pltpu.make_async_remote_copy(
            src_ref=r_all.at[r_rows, :], dst_ref=r_all.at[r_rows, :], send_sem=f_send, recv_sem=f_recv,
            device_id=(g, me), device_id_type=MESH_IDS,
        ).start()
    many = r_all.at[pl.ds(0, (groups - 1) * r_cols), :]
    pltpu.make_async_copy(many, many, f_recv).wait()
    pltpu.make_async_copy(many, many, f_send).wait()
    for c in range(orr.shape[0] // 128):
        span = slice(c * 128, (c + 1) * 128)
        orr[span, :] = r_all[:, span].astype(jnp.float32).T.astype(jnp.bfloat16)

    def drain(e, carry):
        for a in range(2):
            wait_sends(a, e)
        return carry

    lax.fori_loop(max(experts - SLOTS, 0), experts, drain, 0)

    def arrive(e, carry):
        for a in range(2):
            many = outs[a].at[e, :, pl.ds(0, (n - 1) * rows)]
            pltpu.make_async_copy(many, many, recv.at[a, e]).wait()
        return carry

    lax.fori_loop(0, experts, arrive, 0)


PIECES = 4


def put_kernel(gate, up, router, og, ou, orr, done, done_router):
    size = gate.shape[0] // PIECES
    copies = [
        pltpu.make_async_copy(src.at[pl.ds(i * size, size)], dst.at[pl.ds(i * size, size)], done.at[a, i])
        for i in range(PIECES)
        for a, (src, dst) in enumerate(((gate, og), (up, ou)))
    ]
    copies.append(pltpu.make_async_copy(router, orr, done_router))
    for copy in copies:
        copy.start()
    for copy in copies:
        copy.wait()


def put(*held):
    anywhere = pl.BlockSpec(memory_space=pl.ANY)
    return pl.pallas_call(
        put_kernel,
        out_shape=tuple(pltpu.HBM(x.shape, x.dtype) for x in held),
        in_specs=[anywhere] * len(held),
        out_specs=(anywhere,) * len(held),
        scratch_shapes=[pltpu.SemaphoreType.DMA((2, PIECES)), pltpu.SemaphoreType.DMA],
        compiler_params=pltpu.CompilerParams(vmem_limit_bytes=1024 * 1024),
        name="put",
    )(*held)


def fused(n, groups, master_gate, second_gate, master_up, second_up, router_weight, router_gain):
    experts, rows, inner = master_gate.shape
    r_cols = router_weight.shape[1]
    final = (experts, inner // n, rows * n)
    anywhere = pl.BlockSpec(memory_space=pl.ANY)
    dma = pltpu.SemaphoreType.DMA
    return put(*pl.pallas_call(
        functools.partial(regroup_kernel, n, groups),
        out_shape=(
            pltpu.VMEM(final, jnp.bfloat16),
            pltpu.VMEM(final, jnp.bfloat16),
            jax.ShapeDtypeStruct((rows * n, r_cols * groups), jnp.bfloat16),
        ),
        in_specs=[anywhere] * 6,
        out_specs=(anywhere, anywhere, pl.BlockSpec(memory_space=pltpu.VMEM)),
        scratch_shapes=[
            pltpu.VMEM((2, LOADS, rows, inner), jnp.float32),
            pltpu.VMEM((2, LOADS, rows, inner), jnp.bfloat16),
            pltpu.VMEM((2, SLOTS, inner, rows), jnp.bfloat16),
            pltpu.VMEM((r_cols, rows), jnp.float32),
            pltpu.VMEM((1, rows), jnp.float32),
            pltpu.VMEM((r_cols, rows), jnp.bfloat16),
            pltpu.VMEM((r_cols * groups, rows * n), jnp.bfloat16),
            dma((2, LOADS)), dma((2, LOADS)), dma((2,)),
            dma((2, SLOTS)), dma((2, SLOTS)), dma((2, experts)),
            dma((3,)), dma((3,)), dma, dma,
        ],
        compiler_params=pltpu.CompilerParams(
            collective_id=0, has_side_effects=True, vmem_limit_bytes=24 * 1024 * 1024,
        ),
        name="regroup",
    )(
        master_gate, second_gate, master_up, second_up,
        pltpu.with_memory_space_constraint(router_weight.T, pltpu.HBM),
        pltpu.with_memory_space_constraint(router_gain[None, :], pltpu.HBM),
    ))


def solution(mesh):
    n, groups = mesh.shape["shard"], mesh.shape["expert"]

    def shards(*args):
        experts, rows, inner = args[0].shape
        r_cols = args[4].shape[1]
        fits = (
            n % 2 == 0 and n > 2 and groups > 1 and rows % 128 == 0 and inner % 128 == 0
            and (inner // n) % 16 == 0 and r_cols % 16 == 0 and experts % PIECES == 0 and experts >= max(SLOTS, LOADS)
        )
        return fused(n, groups, *args) if fits else plain(*args)

    in_specs = (
        P("expert", "shard", None),
        P("expert", "shard", None),
        P("expert", "shard", None),
        P("expert", "shard", None),
        P("shard", "expert"),
        P("shard"),
    )
    out_specs = (P("expert", "shard", None), P("expert", "shard", None), P())
    return jax.shard_map(shards, mesh=mesh, in_specs=in_specs, out_specs=out_specs, check_vma=False)
```
